32 devices in a mesh: groups: 2 (over x), seq: 16 (over z, y, core).
Axes of the slice: x: 2, y: 2, z: 4, core: 2. Of those that a mesh axis runs over, the one named last changes fastest.
Arguments:
- hidden_in: bfloat16 [32768, 2048], P(('groups', 'seq')), parts along dimension 0, may hold values from -6 to 6
- queries: bfloat16 [32768, 1024], P(('groups', 'seq')), parts along dimension 0, may hold values from -6 to 6
- kv_weight: bfloat16 [2048, 2048], replicated, may hold values from -0.125 to 0.125
- level_weight: float32 [16, 8], replicated, may hold values from 0.3 to 3
Outputs:
- attended: bfloat16 [32768, 1024], P(('groups', 'seq')), parts along dimension 0
The draws below stay inside these ranges and needn't reach their ends.
There are 2 independent parts, one for each index of `groups`. The reference program is written for one: setup_inputs(seed, part) draws one part's arguments, and reference() takes and returns one part's arrays. A program takes and returns all parts, laid end to end along the dimension named above; an argument that names none is the same for every part. Nothing has to cross between parts.
All inputs are finite; a program needn't handle non-finite values.
Results may differ from the reference program's by a relative error of at most 0.0034.
Values sent between devices are 32-bit elements; how exact they have to be, the bound alone decides.
A program may use at most 128 MiB of HBM per device.

```python
import math
import jax
import jax.numpy as jnp
from jax import lax

D = 2048
HEADS = 8
HEAD = 128
SPAN = 64
LEVELS = 16
TOKENS = 16384


def steps_of(rng, shape, shards, least, high):
    factor_of = 1.0
    for axis_at, blocks in shards:
        steps = jax.random.uniform(jax.random.fold_in(jax.random.fold_in(rng, 6), axis_at), (blocks,), jnp.float32, least / len(shards), high / len(shards))
        factor_of = factor_of * jnp.repeat(jnp.exp(steps), shape[axis_at] // blocks).reshape((-1,) + (1,) * (len(shape) - 1 - axis_at))
    return factor_of


def noise(stream_key, shape, spread, most, cuts=(), kind=jnp.bfloat16):
    values = spread * jax.random.normal(stream_key, shape, jnp.float32)
    if cuts:
        values = values * steps_of(stream_key, shape, cuts, -0.22, 0.18)
    return jnp.clip(values, -most, most).astype(kind)


def setup_inputs(seed: int = 0, part: int = 0) -> dict:
    streams_of = jax.random.split(jax.random.key(seed), 5)
    part_keys = jax.random.split(jax.random.fold_in(streams_of[4], part), 5)
    hidden_in = noise(part_keys[0], (TOKENS, D), 1.0, 6.0, ((0, 16),))
    queries = noise(part_keys[1], (TOKENS, HEADS * HEAD), 1.0, 6.0, ((0, 16),))
    kv_weight = noise(streams_of[2], (D, 2 * HEADS * HEAD), D ** -0.5, 0.125)
    level_weight = jnp.clip(jnp.exp(jax.random.uniform(streams_of[3], (LEVELS, HEADS), jnp.float32, math.log(0.3), math.log(3.0))), 0.3, 3.0)
    return dict(hidden_in=hidden_in, queries=queries, kv_weight=kv_weight, level_weight=level_weight)


def reference(hidden_in, queries, kv_weight, level_weight):
    tokens = hidden_in.shape[0]
    spans = tokens // SPAN
    width = HEADS * HEAD
    nbits = LEVELS - 1
    highest = lax.Precision.HIGHEST
    kv = jnp.dot(hidden_in, kv_weight, preferred_element_type=jnp.float32).astype(jnp.bfloat16)
    keys = kv[:, :width].reshape(spans, SPAN, HEADS, HEAD)
    values = kv[:, width:].reshape(spans, SPAN, HEADS, HEAD)
    query_blocks = queries.reshape(spans, SPAN, HEADS, HEAD)
    levels = jnp.arange(nbits, dtype=jnp.int32)
    lengths = 2.0 ** levels.astype(jnp.float32) * SPAN
    scales = level_weight[1:] / jnp.sqrt(lengths)[:, None]
    causal = jnp.tril(jnp.ones((SPAN, SPAN), jnp.float32))
    diag_scale = level_weight[0] / jnp.sqrt(jnp.float32(SPAN * HEAD))

    def advance(carry, inputs):
        running, done = carry
        key_c, val_c, query_c, index = inputs
        bits = (jnp.right_shift(index, levels) & 1).astype(jnp.float32)
        coef = bits[:, None] * scales
        state = jnp.einsum('lh,lhab->hab', coef, done, precision=highest)
        query_f = query_c.astype(jnp.float32)
        key_f = key_c.astype(jnp.float32)
        val_f = val_c.astype(jnp.float32)
        inter = jnp.einsum('tha,hab->thb', query_f, state, precision=highest) / jnp.sqrt(jnp.float32(HEAD))
        scores = jnp.einsum('tha,sha->hts', query_f, key_f, precision=highest)
        scores = (scores * diag_scale[:, None, None] * causal[None]).astype(jnp.bfloat16)
        intra = jnp.einsum('hts,shb->thb', scores.astype(jnp.float32), val_f, precision=highest)
        result = (intra + inter).astype(jnp.bfloat16)
        span_state = jnp.einsum('tha,thb->hab', key_f, val_f, precision=highest)
        running = running + span_state[None]
        powers = jnp.left_shift(jnp.int32(1), levels)
        complete = (index + 1) % powers == 0
        done = jnp.where(complete[:, None, None, None], running, done)
        running = jnp.where(complete[:, None, None, None], jnp.zeros_like(running), running)
        return ((running, done), result)
    start = jnp.zeros((nbits, HEADS, HEAD, HEAD), jnp.float32)
    order = jnp.arange(spans, dtype=jnp.int32)
    _, results = lax.scan(advance, (start, start), (keys, values, query_blocks, order))
    return results.reshape(tokens, width)
```

```python
import functools
import math

import jax
import jax.numpy as jnp
from jax import lax
from jax.experimental import pallas as pl
from jax.experimental.pallas import tpu as pltpu
from jax.sharding import PartitionSpec as P

HEADS = 8
HEAD = 128
SPAN = 64
PAIR = 2
MESH = pl.DeviceIdType.MESH
F32 = jnp.float32
BF16 = jnp.bfloat16


def kernel(depth, tokens, block, tile, x_hbm, q_hbm, w_hbm, lw, out_hbm,
           x, w, q, kv, local, out, weight, states, total, near, away, sums, got,
           x_sem, w_sem, q_sem, out_sem, near_send, near_recv, far_send, far_recv, share_send, share_recv):
    width = HEADS * HEAD
    wide = PAIR * HEAD
    groups = HEADS // PAIR
    blocks = tokens // block
    tiles = tokens // tile
    inner_bits = (block // SPAN).bit_length() - 1
    local_bits = (tokens // SPAN).bit_length() - 1
    index = lax.axis_index("seq")
    core = index & 1
    partners = [index ^ (1 << level) for level in range(depth)]

    barrier = pltpu.get_barrier_semaphore()
    for partner in partners:
        pl.semaphore_signal(barrier, inc=1, device_id={"seq": partner}, device_id_type=MESH)

    def x_copy(i):
        rows = pl.ds(i * tile, tile)
        return pltpu.make_async_copy(x_hbm.at[rows], x.at[rows], x_sem.at[i])

    def w_copy(g, side):
        columns = pl.ds(side * width + g * wide, wide)
        return pltpu.make_async_copy(w_hbm.at[:, columns], w.at[g, side], w_sem.at[g, side])

    q_copy = pltpu.make_async_copy(q_hbm, q, q_sem)

    def out_copy(g):
        columns = pl.ds(g * wide, wide)
        return pltpu.make_async_copy(out.at[:, columns], out_hbm.at[:, columns], out_sem.at[g])

    w_copy(0, 0).start()
    x_copy(0).start()
    w_copy(0, 1).start()
    for i in range(1, tiles):
        x_copy(i).start()
    for g in range(1, groups):
        w_copy(g, 0).start()
        w_copy(g, 1).start()
    q_copy.start()

    def remote(src, dst, send, recv, partner):
        return pltpu.make_async_remote_copy(
            src_ref=src, dst_ref=dst, send_sem=send, recv_sem=recv,
            device_id={"seq": partner}, device_id_type=MESH)

    def near_copy(g):
        return remote(total.at[g], near.at[g], near_send.at[g], near_recv.at[g], partners[0])

    def far_copy(g, level):
        return remote(sums.at[level - 1, g], got.at[level - 1, g], far_send.at[level - 1, g],
                      far_recv.at[level - 1, g], partners[level])

    def share_copy(g):
        return remote(away.at[g, core], away.at[g, core], share_send.at[g], share_recv.at[g], partners[0])

    def factor(level, head):
        return lw[1 + level, head] * (1.0 / math.sqrt(2**level * SPAN))

    def project(g):
        kc = slice(g * wide, (g + 1) * wide)
        vc = slice(width + g * wide, width + (g + 1) * wide)
        w_copy(g, 0).wait()
        w_copy(g, 1).wait()

        def body(i):
            rows = pl.ds(pl.multiple_of(i * tile, tile), tile)
            xt = x[rows, :]
            keys = jnp.dot(xt, w[g, 0], preferred_element_type=F32).astype(BF16)
            values = jnp.dot(xt, w[g, 1], preferred_element_type=F32).astype(BF16)
            kv[rows, kc] = keys
            kv[rows, vc] = values
            for b in range(tile // block):
                part = slice(b * block, (b + 1) * block)
                both = lax.dot_general(keys[part], values[part], (((0,), (0,)), ((), ())),
                                       preferred_element_type=F32)
                for e in range(PAIR):
                    own = slice(e * HEAD, (e + 1) * HEAD)
                    states[g * PAIR + e, i * (tile // block) + b] = both[own, own]

        if g == 0:
            for i in range(tiles):
                x_copy(i).wait()
                body(i)
        else:
            pl.loop(0, tiles)(body)
        for e in range(PAIR):
            total[g, e] = sum(states[g * PAIR + e, b] for b in range(blocks))

    def attend(g):
        if g == 0:
            q_copy.wait()
        target = lax.broadcasted_iota(jnp.int32, (block, block), 0)
        source = lax.broadcasted_iota(jnp.int32, (block, block), 1)
        differ = (target // SPAN) ^ (source // SPAN)
        for e in range(PAIR):
            head = g * PAIR + e
            at = jnp.full((block, block), lw[0, head] * (1.0 / math.sqrt(SPAN * HEAD)), F32)
            for level in range(inner_bits):
                at = jnp.where(differ >= 1 << level, factor(level, head) * (1.0 / math.sqrt(HEAD)), at)
            weight[e] = jnp.where(source <= target, at, 0.0)

        @pl.loop(0, blocks)
        def _(b):
            rows = pl.ds(pl.multiple_of(b * block, block), block)
            for e in range(PAIR):
                head = g * PAIR + e
                columns = slice(head * HEAD, (head + 1) * HEAD)
                keys = kv[rows, columns]
                values = kv[rows, width + head * HEAD:width + (head + 1) * HEAD]
                scores = lax.dot_general(q[rows, columns], keys, (((1,), (1,)), ((), ())),
                                         preferred_element_type=F32)
                scores = (scores * weight[e]).astype(BF16)
                local[rows, columns] = jnp.dot(scores, values, preferred_element_type=F32)

    def finish(g):
        for e in range(PAIR):
            head = g * PAIR + e
            columns = slice(head * HEAD, (head + 1) * HEAD)
            bit = core.astype(F32) * factor(local_bits, head)
            base = away[g, e] + bit * near[g, e]
            for b in range(blocks):
                mixed = base
                for level in range(local_bits - inner_bits):
                    if b >> level & 1:
                        first = (b >> level + 1) << level + 1
                        held = sum(states[head, j] for j in range(first, first + (1 << level)))
                        mixed = mixed + factor(inner_bits + level, head) * held
                mixed = mixed * (1.0 / math.sqrt(HEAD))
                high = mixed.astype(BF16)
                low = (mixed - high.astype(F32)).astype(BF16)
                rows = slice(b * block, (b + 1) * block)
                qb = q[rows, columns]
                inter = jnp.dot(jnp.concatenate([qb, qb], 1), jnp.concatenate([high, low], 0),
                                preferred_element_type=F32)
                out[rows, columns] = (local[rows, columns] + inter).astype(BF16)
        out_copy(g).start()

    def stage(g, s):
        if s == 0:
            if g == 0:
                pl.semaphore_wait(barrier, depth)
            near_copy(g).start()
        elif s == 1:
            near_copy(g).wait()
            if depth > 1:
                sums[0, g] = total[g, core] + near[g, core]
                far_copy(g, 1).start()
        elif s <= depth:
            level = s - 1
            far_copy(g, level).wait()
            bit = (jnp.right_shift(index, level) & 1).astype(F32)
            term = (bit * factor(local_bits + level, g * PAIR + core)) * got[level - 1, g]
            away[g, core] = term if level == 1 else away[g, core] + term
            if level + 1 < depth:
                sums[level, g] = sums[level - 1, g] + got[level - 1, g]
                far_copy(g, level + 1).start()
            else:
                share_copy(g).start()
        else:
            share_copy(g).wait()
            finish(g)

    for slot in range(2 * groups + depth + 1):
        if slot < groups:
            project(slot)
        elif slot < 2 * groups:
            attend(slot - groups)
        for g in range(groups):
            lag = slot - g
            if slot >= groups and g == groups - 1:
                lag = slot - g
            if 0 <= lag <= depth:
                stage(g, lag)
            if slot >= 2 * groups - 1 and lag == max(depth + 1, 2 * groups - 1 - g):
                stage(g, depth + 1)
    for g in range(groups):
        out_copy(g).wait()


def local(depth, x, q, w, lw):
    tokens, width = q.shape
    groups = HEADS // PAIR
    block = min(256, tokens)
    tile = min(512, tokens)
    levels = max(depth - 1, 1)
    dma = pltpu.SemaphoreType.DMA
    hbm = pl.BlockSpec(memory_space=pl.ANY)
    return pl.pallas_call(
        functools.partial(kernel, depth, tokens, block, tile),
        out_shape=jax.ShapeDtypeStruct((tokens, width), BF16),
        in_specs=[hbm, hbm, hbm, pl.BlockSpec(memory_space=pltpu.SMEM)],
        out_specs=hbm,
        scratch_shapes=[
            pltpu.VMEM(x.shape, BF16),
            pltpu.VMEM((groups, 2, w.shape[0], PAIR * HEAD), BF16),
            pltpu.VMEM(q.shape, BF16),
            pltpu.VMEM((tokens, 2 * width), BF16),
            pltpu.VMEM((tokens, width), F32),
            pltpu.VMEM((tokens, width), BF16),
            pltpu.VMEM((PAIR, block, block), F32),
            pltpu.VMEM((HEADS, tokens // block, HEAD, HEAD), F32),
            pltpu.VMEM((groups, PAIR, HEAD, HEAD), F32),
            pltpu.VMEM((groups, PAIR, HEAD, HEAD), F32),
            pltpu.VMEM((groups, PAIR, HEAD, HEAD), F32),
            pltpu.VMEM((levels, groups, HEAD, HEAD), F32),
            pltpu.VMEM((levels, groups, HEAD, HEAD), F32),
            dma((tokens // tile,)), dma((groups, 2)), dma, dma((groups,)),
            dma((groups,)), dma((groups,)), dma((levels, groups)), dma((levels, groups)),
            dma((groups,)), dma((groups,)),
        ],
        compiler_params=pltpu.CompilerParams(collective_id=0, has_side_effects=True),
    )(x, q, w, lw)


def solution(mesh):
    depth = mesh.shape["seq"].bit_length() - 1
    rows = P(("groups", "seq"), None)
    return jax.shard_map(functools.partial(local, depth), mesh=mesh, in_specs=(rows, rows, P(), P()),
                         out_specs=rows, check_vma=False)
```

```python
import functools
import math

import jax
import jax.numpy as jnp
from jax import lax
from jax.experimental import pallas as pl
from jax.experimental.pallas import tpu as pltpu
from jax.sharding import PartitionSpec as P

HEADS = 8
HEAD = 128
SPAN = 64
PAIR = 2
MESH = pl.DeviceIdType.MESH
F32 = jnp.float32
BF16 = jnp.bfloat16


def kernel(depth, tokens, block, tile, x_hbm, q_hbm, w_hbm, lw_hbm, out_hbm,
           x, w, q, kv, local, out, weight, states, total, near, away, sums, got,
           lw, lw_sem, x_sem, w_sem, q_sem, out_sem, near_send, near_recv, far_send, far_recv, share_send, share_recv):
    width = HEADS * HEAD
    wide = PAIR * HEAD
    groups = HEADS // PAIR
    blocks = tokens // block
    tiles = tokens // tile
    inner_bits = (block // SPAN).bit_length() - 1
    local_bits = (tokens // SPAN).bit_length() - 1
    index = lax.axis_index("seq")
    core = index & 1
    partners = [index ^ (1 << level) for level in range(depth)]

    barrier = pltpu.get_barrier_semaphore()
    for partner in partners:
        pl.semaphore_signal(barrier, inc=1, device_id={"seq": partner}, device_id_type=MESH)

    def x_copy(i):
        rows = pl.ds(i * tile, tile)
        return pltpu.make_async_copy(x_hbm.at[rows], x.at[rows], x_sem.at[i])

    def w_copy(g, side):
        columns = pl.ds(side * width + g * wide, wide)
        return pltpu.make_async_copy(w_hbm.at[:, columns], w.at[g, side], w_sem.at[g, side])

    q_copy = pltpu.make_async_copy(q_hbm, q, q_sem)

    def out_copy(g):
        columns = pl.ds(g * wide, wide)
        return pltpu.make_async_copy(out.at[:, columns], out_hbm.at[:, columns], out_sem.at[g])

    lw_copy = pltpu.make_async_copy(lw_hbm, lw, lw_sem)
    w_copy(0, 0).start()
    x_copy(0).start()
    w_copy(0, 1).start()
    for i in range(1, tiles):
        x_copy(i).start()
    for g in range(1, groups):
        w_copy(g, 0).start()
        w_copy(g, 1).start()
    q_copy.start()
    lw_copy.start()

    def remote(src, dst, send, recv, partner):
        return pltpu.make_async_remote_copy(
            src_ref=src, dst_ref=dst, send_sem=send, recv_sem=recv,
            device_id={"seq": partner}, device_id_type=MESH)

    def near_copy(g):
        return remote(total.at[g], near.at[g], near_send.at[g], near_recv.at[g], partners[0])

    def far_copy(g, level):
        return remote(sums.at[level - 1, g], got.at[level - 1, g], far_send.at[level - 1, g],
                      far_recv.at[level - 1, g], partners[level])

    def share_copy(g):
        return remote(away.at[g, core], away.at[g, core], share_send.at[g], share_recv.at[g], partners[0])

    def entry(row, head):
        return lw[row:row + 1, head:head + 1]

    def factor(level, head):
        return entry(1 + level, head) * (1.0 / math.sqrt(2**level * SPAN))

    def project(g):
        kc = slice(g * wide, (g + 1) * wide)
        vc = slice(width + g * wide, width + (g + 1) * wide)
        w_copy(g, 0).wait()
        w_copy(g, 1).wait()

        def body(i):
            rows = pl.ds(pl.multiple_of(i * tile, tile), tile)
            xt = x[rows, :]
            keys = jnp.dot(xt, w[g, 0], preferred_element_type=F32).astype(BF16)
            values = jnp.dot(xt, w[g, 1], preferred_element_type=F32).astype(BF16)
            kv[rows, kc] = keys
            kv[rows, vc] = values
            for b in range(tile // block):
                part = slice(b * block, (b + 1) * block)
                both = lax.dot_general(keys[part], values[part], (((0,), (0,)), ((), ())),
                                       preferred_element_type=F32)
                for e in range(PAIR):
                    own = slice(e * HEAD, (e + 1) * HEAD)
                    states[g * PAIR + e, i * (tile // block) + b] = both[own, own]

        if g == 0:
            lw_copy.wait()
            for i in range(tiles):
                x_copy(i).wait()
                body(i)
        else:
            pl.loop(0, tiles)(body)
        for e in range(PAIR):
            total[g, e] = sum(states[g * PAIR + e, b] for b in range(blocks))

    def attend(g):
        if g == 0:
            q_copy.wait()
        target = lax.broadcasted_iota(jnp.int32, (block, block), 0)
        source = lax.broadcasted_iota(jnp.int32, (block, block), 1)
        differ = (target // SPAN) ^ (source // SPAN)
        for e in range(PAIR):
            head = g * PAIR + e
            at = jnp.broadcast_to(entry(0, head) * (1.0 / math.sqrt(SPAN * HEAD)), (block, block))
            for level in range(inner_bits):
                at = jnp.where(differ >= 1 << level, factor(level, head) * (1.0 / math.sqrt(HEAD)), at)
            weight[e] = jnp.where(source <= target, at, 0.0)

        for b in range(blocks):
            rows = slice(b * block, (b + 1) * block)
            for e in range(PAIR):
                head = g * PAIR + e
                columns = slice(head * HEAD, (head + 1) * HEAD)
                keys = kv[rows, columns]
                values = kv[rows, width + head * HEAD:width + (head + 1) * HEAD]
                scores = lax.dot_general(q[rows, columns], keys, (((1,), (1,)), ((), ())),
                                         preferred_element_type=F32)
                scores = (scores * weight[e]).astype(BF16)
                local[rows, columns] = jnp.dot(scores, values, preferred_element_type=F32)

    def finish(g):
        for e in range(PAIR):
            head = g * PAIR + e
            columns = slice(head * HEAD, (head + 1) * HEAD)
            bit = core.astype(F32) * factor(local_bits, head)
            base = away[g, e] + bit * near[g, e]
            for b in range(blocks):
                mixed = base
                for level in range(local_bits - inner_bits):
                    if b >> level & 1:
                        first = (b >> level + 1) << level + 1
                        held = sum(states[head, j] for j in range(first, first + (1 << level)))
                        mixed = mixed + factor(inner_bits + level, head) * held
                mixed = mixed * (1.0 / math.sqrt(HEAD))
                high = mixed.astype(BF16)
                low = (mixed - high.astype(F32)).astype(BF16)
                rows = slice(b * block, (b + 1) * block)
                qb = q[rows, columns]
                inter = jnp.dot(jnp.concatenate([qb, qb], 1), jnp.concatenate([high, low], 0),
                                preferred_element_type=F32)
                out[rows, columns] = (local[rows, columns] + inter).astype(BF16)
        out_copy(g).start()

    def stage(g, s):
        if s == 0:
            if g == 0:
                pl.semaphore_wait(barrier, depth)
            near_copy(g).start()
        elif s == 1:
            near_copy(g).wait()
            if depth > 1:
                sums[0, g] = total[g, core] + near[g, core]
                far_copy(g, 1).start()
        elif s <= depth:
            level = s - 1
            far_copy(g, level).wait()
            bit = (jnp.right_shift(index, level) & 1).astype(F32)
            scale = jnp.where(core == 0, factor(local_bits + level, g * PAIR), factor(local_bits + level, g * PAIR + 1))
            term = (bit * scale) * got[level - 1, g]
            away[g, core] = term if level == 1 else away[g, core] + term
            if level + 1 < depth:
                sums[level, g] = sums[level - 1, g] + got[level - 1, g]
                far_copy(g, level + 1).start()
            else:
                share_copy(g).start()
        else:
            share_copy(g).wait()
            finish(g)

    last = max(depth + 4, 2 * groups)
    for slot in range(groups + last):
        if slot < groups:
            project(slot)
        elif slot < 2 * groups:
            attend(slot - groups)
        for g in reversed(range(groups)):
            lag = slot - g
            if 0 <= lag < depth:
                stage(g, lag)
            elif lag == depth + 2:
                stage(g, depth)
            elif lag == last:
                stage(g, depth + 1)
    for g in range(groups):
        out_copy(g).wait()


def local(depth, x, q, w, lw):
    tokens, width = q.shape
    groups = HEADS // PAIR
    block = min(256, tokens)
    tile = min(1024, tokens)
    levels = max(depth - 1, 1)
    dma = pltpu.SemaphoreType.DMA
    hbm = pl.BlockSpec(memory_space=pl.ANY)
    return pl.pallas_call(
        functools.partial(kernel, depth, tokens, block, tile),
        out_shape=jax.ShapeDtypeStruct((tokens, width), BF16),
        in_specs=[hbm, hbm, hbm, hbm],
        out_specs=hbm,
        scratch_shapes=[
            pltpu.VMEM(x.shape, BF16),
            pltpu.VMEM((groups, 2, w.shape[0], PAIR * HEAD), BF16),
            pltpu.VMEM(q.shape, BF16),
            pltpu.VMEM((tokens, 2 * width), BF16),
            pltpu.VMEM((tokens, width), F32),
            pltpu.VMEM((tokens, width), BF16),
            pltpu.VMEM((PAIR, block, block), F32),
            pltpu.VMEM((HEADS, tokens // block, HEAD, HEAD), F32),
            pltpu.VMEM((groups, PAIR, HEAD, HEAD), F32),
            pltpu.VMEM((groups, PAIR, HEAD, HEAD), F32),
            pltpu.VMEM((groups, PAIR, HEAD, HEAD), F32),
            pltpu.VMEM((levels, groups, HEAD, HEAD), F32),
            pltpu.VMEM((levels, groups, HEAD, HEAD), F32),
            pltpu.VMEM(lw.shape, F32),
            dma, dma((tokens // tile,)), dma((groups, 2)), dma, dma((groups,)),
            dma((groups,)), dma((groups,)), dma((levels, groups)), dma((levels, groups)),
            dma((groups,)), dma((groups,)),
        ],
        compiler_params=pltpu.CompilerParams(collective_id=0, has_side_effects=True),
    )(x, q, w, lw)


def solution(mesh):
    depth = mesh.shape["seq"].bit_length() - 1
    rows = P(("groups", "seq"), None)
    return jax.shard_map(functools.partial(local, depth), mesh=mesh, in_specs=(rows, rows, P(), P()),
                         out_specs=rows, check_vma=False)
```
